32 devices in a mesh: row: 8 (over z, x), col: 4 (over y, core).
Axes of the slice: x: 2, y: 2, z: 4, core: 2. Of those that a mesh axis runs over, the one named last changes fastest.
Arguments:
- samples: float32 [4096, 512], P(('row', 'col')), may hold values from -8 to 8
- labels: int32 [4096, 256], P(('row', 'col')), may hold values from -1 to 1, as said below
Outputs:
- statistic: float32 [256], replicated
- proof: float32 [4096], P(('row', 'col'))
- p_value: float32 [], replicated
The draws below stay inside these ranges and needn't reach their ends.
Inputs may be any that keep to these rules, and one draw needn't show every extreme that they name: `labels`: every column holds exactly 2048 entries +1 and 2048 entries -1.
All inputs are finite; a program needn't handle non-finite values.
Results may differ from the reference program's by a relative error of at most 0.0003.
Values sent between devices are 32-bit elements; how exact they have to be, the bound alone decides.
A program may use at most 64 MiB of HBM per device.

```python
import math
import jax
import jax.numpy as jnp
from jax import lax

W = 512
PERMS = 256
NS = 4096


def draw_samples(key, part):
    base = jax.random.fold_in(key, 11)
    member_key, center_key, spread_key, jitter_key, scale_key = jax.random.split(base, 5)
    member = jax.random.randint(member_key, (NS,), 0, 128)
    spread = jnp.exp(jax.random.uniform(spread_key, (128, 1), jnp.float32, jnp.log(0.7), jnp.log(2.5)))
    scales = jnp.exp(jax.random.uniform(scale_key, (NS, 1), jnp.float32, jnp.log(0.25), jnp.log(1.0)))
    centers = jnp.clip(jax.random.normal(center_key, (128, W), jnp.float32), -2.5, 2.5)
    jitter = jnp.clip(jax.random.normal(jitter_key, (NS, W), jnp.float32), -1.5, 1.5)
    placed = (centers * spread)[member]
    return (placed + jitter * scales).astype(jnp.float32)


def draw_labels(key, part):
    keys = jax.random.split(jax.random.fold_in(key, 23), PERMS)
    orders = jax.vmap(lambda one: jax.random.permutation(one, NS))(keys)
    return jnp.where(orders < NS // 2, 1, -1).astype(jnp.int32).T


def setup_inputs(seed: int = 0) -> dict:
    key_list = jax.random.split(jax.random.key(seed), 3)
    return {
        "samples": draw_samples(jax.random.fold_in(key_list[2], 71), 0),
        "labels": draw_labels(jax.random.fold_in(key_list[2], 71), 0),
    }


def tile_terms(xr, lr, gr, xc, lc, gc, width):
    norm_rows = lax.optimization_barrier(jnp.sum(xr * xr, 1))
    norm_cols = lax.optimization_barrier(jnp.sum(xc * xc, 1))
    dots = lax.dot_general(xr, xc, (((1,), (1,)), ((), ())), precision=lax.Precision.HIGHEST, preferred_element_type=jnp.float32)
    dist = jnp.maximum(norm_rows[:, None] + norm_cols[None, :] - 2.0 * dots, 0.0)
    kern = jnp.where(gr[:, None] == gc[None, :], 0.0, jnp.exp(-dist / (2.0 * width)))
    proj = jnp.dot(kern, lc, precision=lax.Precision.HIGHEST, preferred_element_type=jnp.float32)
    return (proj[:, 0], lax.optimization_barrier(jnp.sum(lr * proj, 0)), jnp.sum(kern))

def reference(samples, labels):
    total_rows = samples.shape[0]
    width = samples.shape[1]
    perms = labels.shape[1]
    labs = labels.astype(jnp.float32)
    tile = math.gcd(total_rows, 1024)
    count = total_rows // tile
    ids = jnp.arange(total_rows, dtype=jnp.int32)

    def one(args):
        xr, lr, gr = args
        return tile_terms(xr, lr, gr, samples, labs, ids, width)
    wit, quad, tot = lax.map(one, (samples.reshape(count, tile, width), labs.reshape(count, tile, perms), ids.reshape(count, tile)))
    quad = lax.optimization_barrier(jnp.sum(quad, 0))
    total = jnp.sum(tot)
    half = total_rows / 2.0
    statistic = total / (2.0 * half * (half - 1.0)) + (2.0 * half - 1.0) / (2.0 * half * (half - 1.0)) * quad
    proof = wit.reshape(total_rows) / jnp.sqrt(jnp.float32(total_rows))
    p_value = jnp.mean(jax.nn.sigmoid(4.0 * (statistic[1:] - statistic[0])))
    return (statistic, proof, p_value)
```

```python
import functools
import math

import jax
import jax.numpy as jnp
from jax import lax
from jax.experimental import pallas as pl
from jax.experimental.pallas import tpu as pltpu
from jax.sharding import PartitionSpec as P

MESH = pl.DeviceIdType.MESH
F32 = jnp.float32
BF16 = jnp.bfloat16
CHUNKS = 4
PARTS = 2

ROUTES = {1: {}, 2: {0: (1, 1)}, 4: {0: (1, 3), 2: (-1, 1), 3: (-1, 2)}}


def nt(a, b):
    return lax.dot_general(a, b, (((1,), (1,)), ((), ())), preferred_element_type=F32)


def nn(a, b):
    return lax.dot_general(a, b, (((1,), (0,)), ((), ())), preferred_element_type=F32)


def split(v):
    hi = v.astype(BF16)
    return hi, (v - hi.astype(F32)).astype(BF16)


def to_row(column):
    n = column.shape[0]
    return jnp.transpose(jnp.broadcast_to(column, (n, n)))[0:1, :]


class Plan:
    def __init__(self, n_row, n_col, blk, width, perms):
        self.nz = math.gcd(n_row, 4)
        self.nx = n_row // self.nz
        self.nk = math.gcd(n_col, 2)
        self.ny = n_col // self.nk
        self.n_col = n_col
        self.n_lev = self.nx * n_col
        self.blk, self.width, self.perms = blk, width, perms
        self.group = math.gcd(self.n_lev, 4)
        self.rows = blk * n_row * n_col


def kernel(pn, n_send, x_ref, l_ref, stat_ref, proof_ref, p_ref, RX, RL, CX, CL, RHI, RLO, RLB, NR,
           ROWP, QUAD, TOT, COLP, S1, R1, S2, R2, send, lev_sem, z_sem, s1_send, s1_recv, s2_send, s2_recv):
    nx, ny, nz, nk, n_col, n_lev, blk = pn.nx, pn.ny, pn.nz, pn.nk, pn.n_col, pn.n_lev, pn.blk
    row, col = lax.axis_index("row"), lax.axis_index("col")
    z, x = row // nx, row % nx
    y, core = col // nk, col % nk
    me = x * n_col + col
    routes = ROUTES[nz]
    pending = []

    def lev_of(xx, yy, kk):
        return xx * n_col + yy * nk + kk

    def dev(zz, xx, yy, kk):
        return (zz * nx + xx, yy * nk + kk)

    def lev_dev(k):
        return (z * nx + k // n_col, k % n_col)

    barrier = pltpu.get_barrier_semaphore()
    for d in range(1, n_lev):
        pl.semaphore_signal(barrier, inc=1, device_id=lev_dev((me + d) % n_lev), device_id_type=MESH)
    for d in range(1, nz):
        pl.semaphore_signal(barrier, inc=1, device_id=dev((z + d) % nz, x, y, core), device_id_type=MESH)
    pl.semaphore_wait(barrier, n_lev - 1 + nz - 1)

    counter = [0]

    def new_sem():
        counter[0] += 1
        return send.at[counter[0] - 1]

    half = blk // PARTS
    piece = blk // CHUNKS

    def lev_copy(k, part, target, own, sem):
        r = pl.ds(part * half, half)
        out = []
        for i, (src, dst) in enumerate(((x_ref, RX), (l_ref, RL))):
            s = src.at[r] if own else dst.at[k, r]
            out.append(pltpu.make_async_remote_copy(
                src_ref=s, dst_ref=dst.at[k, r], send_sem=new_sem() if sem else send.at[0],
                recv_sem=lev_sem.at[k, part * 2 + i], device_id=target, device_id_type=MESH))
        return out

    def lev_send(k, part, target, own=False):
        for c in lev_copy(k, part, target, own, True):
            c.start()
            pending.append(c)

    def lev_wait(k, part):
        for c in lev_copy(k, part, (row, col), False, False):
            c.wait_recv()

    def z_copy(b, ch, target, own, sems):
        r = pl.ds(ch * piece, piece)
        out = []
        for i, (src, dst) in enumerate(((x_ref, CX), (l_ref, CL))):
            s = src.at[r] if own else dst.at[b, r]
            out.append(pltpu.make_async_remote_copy(
                src_ref=s, dst_ref=dst.at[b, r], send_sem=sems[i],
                recv_sem=z_sem.at[b, ch * 2 + i], device_id=target, device_id_type=MESH))
        return out

    z_pending = []

    def z_send(b, ch, at, own):
        sems = [new_sem(), new_sem()]
        to = at + routes[b][0]

        @pl.when(z == at)
        def _():
            for c in z_copy(b, ch, dev(to, x, y, core), own, sems):
                c.start()
        z_pending.append((b, ch, at, own, sems))

    def z_event(b, ch, hop):
        at = b + routes[b][0] * hop

        @pl.when(z == at)
        def _():
            for c in z_copy(b, ch, (row, col), False, [send.at[0]] * 2):
                c.wait_recv()
        if hop < routes[b][1]:
            z_send(b, ch, at, False)

    def xm(d):
        return (x + d) % nx

    def ym(d):
        return (y + d) % ny

    other = (core + 1) % nk
    A, B = 0, 1
    for ch in range(CHUNKS):
        for b in routes:
            z_send(b, ch, b, True)
    for d in range(1, nx):
        lev_send(me, A, dev(z, xm(d), y, core), True)
    for d in range(1, ny):
        lev_send(me, B, dev(z, x, ym(d), core), True)
    for d in range(1, nx):
        lev_send(me, B, dev(z, xm(d), y, core), True)
    for d in range(1, ny):
        lev_send(me, A, dev(z, x, ym(d), core), True)
    if nk > 1:
        for part in (A, B):
            lev_send(me, part, dev(z, x, y, other), True)

    def prep(k, xv, lv):
        rows = pl.ds(pl.multiple_of(k * blk, blk), blk)
        hi, lo = split(xv)
        RHI[rows, :] = hi
        RLO[rows, :] = lo
        RLB[rows, :] = lv.astype(F32).astype(BF16)
        NR[:, rows] = to_row(jnp.sum(xv * xv, axis=1, keepdims=True))

    prep(me, x_ref[...], l_ref[...])

    def hops(b):
        return routes[b][1]

    def z_round(hop, ch):
        for b in routes:
            if hop <= hops(b):
                z_event(b, ch, hop)

    z_round(1, 0)
    for d in range(1, nx):
        k = lev_of(xm(d), y, core)
        lev_wait(k, A)
        for e in range(1, ny):
            lev_send(k, A, dev(z, x, ym(e), core))
        if nk > 1:
            lev_send(k, A, dev(z, x, y, other))
    for d in range(1, ny):
        k = lev_of(x, ym(d), core)
        lev_wait(k, B)
        for e in range(1, nx):
            lev_send(k, B, dev(z, xm(e), y, core))
        if nk > 1:
            lev_send(k, B, dev(z, x, y, other))
    z_round(1, 1)
    z_round(2, 0)
    z_round(1, 2)
    z_round(2, 1)
    z_round(1, 3)
    z_round(3, 0)
    for d in range(1, nx):
        k = lev_of(xm(d), y, core)
        lev_wait(k, B)
        if nk > 1:
            lev_send(k, B, dev(z, x, y, other))
    for d in range(1, ny):
        k = lev_of(x, ym(d), core)
        lev_wait(k, A)
        if nk > 1:
            lev_send(k, A, dev(z, x, y, other))
    z_round(2, 2)
    z_round(3, 1)
    z_round(2, 3)
    for d in range(1, nx):
        for e in range(1, ny):
            k = lev_of(xm(d), ym(e), core)
            for part in (A, B):
                lev_wait(k, part)
                if nk > 1:
                    lev_send(k, part, dev(z, x, y, other))
    z_round(3, 2)
    z_round(3, 3)
    if nk > 1:
        for d in range(nx):
            for e in range(ny):
                k = lev_of(xm(d), ym(e), other)
                for part in (A, B):
                    lev_wait(k, part)

    def prep_step(d, _):
        k = (me + d) % n_lev
        prep(k, RX[k], RL[k])
        return 0

    lax.fori_loop(1, n_lev, prep_step, 0)

    span = pn.group * blk
    scale = -1.0 / (2.0 * pn.width)

    def column(xv, lv, own):
        chi, clo = split(xv)
        nc = jnp.sum(xv * xv, axis=1, keepdims=True)
        lf = lv.astype(F32)
        l0 = lf[:, 0:1]
        proj = jnp.zeros((blk, pn.perms), F32)
        tot = jnp.zeros((1, blk), F32)
        for j in range(n_lev // pn.group):
            rows = pl.ds(j * span, span)
            hi, lo, lb = RHI[rows, :], RLO[rows, :], RLB[rows, :]
            dots = nt(chi, hi) + nt(chi, lo) + nt(clo, hi)
            dist = jnp.maximum(nc + NR[:, rows] - 2.0 * dots, 0.0)
            kern = jnp.exp(dist * scale)
            if own:
                ids = lax.broadcasted_iota(jnp.int32, (blk, span), 1) + j * span
                mine = lax.broadcasted_iota(jnp.int32, (blk, span), 0) + me * blk
                kern = jnp.where(ids == mine, 0.0, kern)
            kh, kl = split(kern)
            proj = proj + nn(kh, lb) + nn(kl, lb)
            t = jnp.sum(kern, axis=0, keepdims=True)
            for g in range(pn.group):
                tot = tot + t[:, g * blk:(g + 1) * blk]
            if not own:
                ROWP[:, rows] += jnp.sum(kern * l0, axis=0, keepdims=True)
        quad = jnp.sum(lf * proj, axis=0, keepdims=True)
        return quad, tot, to_row(proj[:, 0:1])

    ROWP[...] = jnp.zeros_like(ROWP)
    COLP[...] = jnp.zeros_like(COLP)
    quad, tot, own_proof = column(x_ref[...], l_ref[...], True)
    QUAD[...] = quad
    TOT[...] = tot
    for b in routes:
        d, h = routes[b]
        reach = [b + d * i for i in range(1, h + 1)]

        @pl.when((z >= min(reach)) & (z <= max(reach)))
        def _():
            q, t, pr = column(CX[b], CL[b], False)
            QUAD[...] += 2.0 * q
            TOT[...] += 2.0 * t
            COLP[b:b + 1, :] = pr

    qr = pn.perms // 128
    for k in range(n_lev):
        for i in range(qr):
            S1[k, i:i + 1, :] = QUAD[:, i * 128:(i + 1) * 128]
        S1[k, qr:qr + 1, :] = TOT[...]
        S1[k, qr + 1:qr + 2, :] = ROWP[:, k * blk:(k + 1) * blk]
        S1[k, qr + 2:, :] = jnp.zeros((S1.shape[1] - qr - 2, 128), F32)

    def s1_copy(d):
        k = (me + d) % n_lev
        return pltpu.make_async_remote_copy(
            src_ref=S1.at[k], dst_ref=R1.at[me], send_sem=s1_send.at[k], recv_sem=s1_recv.at[me],
            device_id=lev_dev(k), device_id_type=MESH)

    def s1_in(d):
        k = (me + d) % n_lev
        return pltpu.make_async_remote_copy(
            src_ref=S1.at[k], dst_ref=R1.at[k], send_sem=s1_send.at[k], recv_sem=s1_recv.at[k],
            device_id=lev_dev(k), device_id_type=MESH)

    for d in range(1, n_lev):
        s1_copy(d).start()
    acc = S1[me]
    for d in range(1, n_lev):
        s1_in(d).wait_recv()
        acc = acc + R1[(me + d) % n_lev]
    for b in range(nz):
        S2[b, :, :] = acc
        S2[b, qr + 1:qr + 2, :] = COLP[b:b + 1, :]

    def s2_copy(d):
        b = (z + d) % nz
        return pltpu.make_async_remote_copy(
            src_ref=S2.at[b], dst_ref=R2.at[z], send_sem=s2_send.at[b], recv_sem=s2_recv.at[z],
            device_id=dev(b, x, y, core), device_id_type=MESH)

    def s2_in(d):
        b = (z + d) % nz
        return pltpu.make_async_remote_copy(
            src_ref=S2.at[b], dst_ref=R2.at[b], send_sem=s2_send.at[b], recv_sem=s2_recv.at[b],
            device_id=dev(b, x, y, core), device_id_type=MESH)

    for d in range(1, nz):
        s2_copy(d).start()
    for d in range(1, nz):
        s2_in(d).wait_recv()
    tops = []
    extra = jnp.zeros((1, 128), F32)
    for b in range(nz):
        mine = z == b
        tops.append(jnp.where(mine, acc, R2[b]))
        extra = extra + jnp.where(mine, 0.0, R2[b, qr + 1:qr + 2, :])
    done = functools.reduce(lambda u, v: u + v, tops)
    proof = acc[qr + 1:qr + 2, :] + own_proof + extra
    total = jnp.sum(done[qr:qr + 1, :], axis=1, keepdims=True)
    hf = pn.rows / 2.0
    den = 2.0 * hf * (hf - 1.0)
    stat = total / den + ((2.0 * hf - 1.0) / den) * done[0:qr, :]
    stat_ref[...] = stat
    proof_ref[...] = proof / math.sqrt(pn.rows)
    sg = 1.0 / (1.0 + jnp.exp(-4.0 * (stat - stat[0:1, 0:1])))
    first = (lax.broadcasted_iota(jnp.int32, stat.shape, 0) + lax.broadcasted_iota(jnp.int32, stat.shape, 1)) == 0
    sg = jnp.where(first, 0.0, sg)
    p = jnp.sum(jnp.sum(sg, axis=0, keepdims=True), axis=1, keepdims=True) / (pn.perms - 1)
    p_ref[...] = p

    for c in pending:
        c.wait_send()
    for b, ch, at, own, sems in z_pending:
        @pl.when(z == at)
        def _():
            for c in z_copy(b, ch, dev(at + routes[b][0], x, y, core), own, sems):
                c.wait_send()
    for d in range(1, n_lev):
        s1_copy(d).wait_send()
    for d in range(1, nz):
        s2_copy(d).wait_send()
    assert counter[0] == n_send


def send_count(pn):
    nx, ny, nk, nz = pn.nx, pn.ny, pn.nk, pn.nz
    own = 2 * (nx - 1) + 2 * (ny - 1) + (2 if nk > 1 else 0)
    fwd = 2 * (nx - 1) * (ny - 1)
    core = 2 * (nx * ny - 1) if nk > 1 else 0
    line = sum(h for _, h in ROUTES[nz].values()) * CHUNKS
    return 2 * (own + fwd + core + line)


def solution(mesh):
    n_row, n_col = mesh.shape["row"], mesh.shape["col"]

    def shards(samples, labels):
        blk, width = samples.shape
        perms = labels.shape[1]
        pn = Plan(n_row, n_col, blk, width, perms)
        n_send = send_count(pn)
        n_lev, nz = pn.n_lev, pn.nz
        vm = pl.BlockSpec(memory_space=pltpu.VMEM)
        dma = pltpu.SemaphoreType.DMA
        stat, proof, p = pl.pallas_call(
            functools.partial(kernel, pn, n_send),
            out_shape=(
                jax.ShapeDtypeStruct((perms // 128, 128), F32),
                jax.ShapeDtypeStruct((1, blk), F32),
                jax.ShapeDtypeStruct((1, 1), F32),
            ),
            in_specs=[vm, vm],
            out_specs=(vm, vm, vm),
            scratch_shapes=[
                pltpu.VMEM((n_lev, blk, width), F32),
                pltpu.VMEM((n_lev, blk, perms), jnp.int32),
                pltpu.VMEM((nz, blk, width), F32),
                pltpu.VMEM((nz, blk, perms), jnp.int32),
                pltpu.VMEM((n_lev * blk, width), BF16),
                pltpu.VMEM((n_lev * blk, width), BF16),
                pltpu.VMEM((n_lev * blk, perms), BF16),
                pltpu.VMEM((1, n_lev * blk), F32),
                pltpu.VMEM((1, n_lev * blk), F32),
                pltpu.VMEM((1, perms), F32),
                pltpu.VMEM((1, blk), F32),
                pltpu.VMEM((nz, blk), F32),
                pltpu.VMEM((n_lev, 8, 128), F32),
                pltpu.VMEM((n_lev, 8, 128), F32),
                pltpu.VMEM((nz, 8, 128), F32),
                pltpu.VMEM((nz, 8, 128), F32),
                dma((n_send,)),
                dma((n_lev, 2 * PARTS)),
                dma((nz, 2 * CHUNKS)),
                dma((n_lev,)),
                dma((n_lev,)),
                dma((nz,)),
                dma((nz,)),
            ],
            compiler_params=pltpu.CompilerParams(
                collective_id=0, has_side_effects=True, vmem_limit_bytes=60 * 1024 * 1024
            ),
        )(samples, labels)
        return stat.reshape(perms), proof.reshape(blk), p.reshape(())

    placed = (P(("row", "col"), None), P(("row", "col"), None))
    return jax.shard_map(
        shards, mesh=mesh, in_specs=placed, out_specs=(P(), P(("row", "col")), P()), check_vma=False
    )
```

```python
import functools
import math

import jax
import jax.numpy as jnp
from jax import lax
from jax.experimental import pallas as pl
from jax.experimental.pallas import tpu as pltpu
from jax.sharding import PartitionSpec as P

MESH = pl.DeviceIdType.MESH
F32 = jnp.float32
BF16 = jnp.bfloat16
CHUNKS = 4
PARTS = 2

ROUTES = {1: {}, 2: {0: (1, 1)}, 4: {0: (1, 3), 2: (-1, 1), 3: (-1, 2)}}


def nt(a, b):
    return lax.dot_general(a, b, (((1,), (1,)), ((), ())), preferred_element_type=F32)


def nn(a, b):
    return lax.dot_general(a, b, (((1,), (0,)), ((), ())), preferred_element_type=F32)


def split(v):
    hi = v.astype(BF16)
    return hi, (v - hi.astype(F32)).astype(BF16)


def to_row(column):
    n = column.shape[0]
    return jnp.transpose(jnp.broadcast_to(column, (n, n)))[0:1, :]


class Plan:
    def __init__(self, n_row, n_col, blk, width, perms):
        self.nz = math.gcd(n_row, 4)
        self.nx = n_row // self.nz
        self.nk = math.gcd(n_col, 2)
        self.ny = n_col // self.nk
        self.n_col = n_col
        self.n_lev = self.nx * n_col
        self.blk, self.width, self.perms = blk, width, perms
        self.group = math.gcd(n_col, 4)
        self.rows = blk * n_row * n_col


def kernel(pn, n_send, x_ref, l_ref, stat_ref, proof_ref, p_ref, RX, RL, CX, CL, RHI, RLO, RLB, NR,
           ROWP, PROJ, QUAD, TOT, COLP, S1, R1, S2, R2, send, lev_sem, z_sem, s1_send, s1_recv, s2_send, s2_recv):
    nx, ny, nz, nk, n_col, n_lev, blk = pn.nx, pn.ny, pn.nz, pn.nk, pn.n_col, pn.n_lev, pn.blk
    row, col = lax.axis_index("row"), lax.axis_index("col")
    z, x = row // nx, row % nx
    y, core = col // nk, col % nk
    me = x * n_col + col
    routes = ROUTES[nz]
    pending = []

    def lev_of(xx, yy, kk):
        return xx * n_col + yy * nk + kk

    def dev(zz, xx, yy, kk):
        return (zz * nx + xx, yy * nk + kk)

    def lev_dev(k):
        return (z * nx + k // n_col, k % n_col)

    barrier = pltpu.get_barrier_semaphore()
    for d in range(1, n_lev):
        pl.semaphore_signal(barrier, inc=1, device_id=lev_dev((me + d) % n_lev), device_id_type=MESH)
    for d in range(1, nz):
        pl.semaphore_signal(barrier, inc=1, device_id=dev((z + d) % nz, x, y, core), device_id_type=MESH)
    pl.semaphore_wait(barrier, n_lev - 1 + nz - 1)

    counter = [0]

    def new_sem():
        counter[0] += 1
        return send.at[counter[0] - 1]

    half = blk // PARTS
    piece = blk // CHUNKS

    def lev_copy(k, part, target, own, sem):
        r = pl.ds(part * half, half)
        out = []
        for i, (src, dst) in enumerate(((x_ref, RX), (l_ref, RL))):
            s = src.at[r] if own else dst.at[k, r]
            out.append(pltpu.make_async_remote_copy(
                src_ref=s, dst_ref=dst.at[k, r], send_sem=new_sem() if sem else send.at[0],
                recv_sem=lev_sem.at[k, part * 2 + i], device_id=target, device_id_type=MESH))
        return out

    def lev_send(k, part, target, own=False):
        for c in lev_copy(k, part, target, own, True):
            c.start()
            pending.append(c)

    def lev_wait(k, part):
        for c in lev_copy(k, part, (row, col), False, False):
            c.wait_recv()

    def z_copy(b, ch, target, own, sems):
        r = pl.ds(ch * piece, piece)
        out = []
        for i, (src, dst) in enumerate(((x_ref, CX), (l_ref, CL))):
            s = src.at[r] if own else dst.at[b, r]
            out.append(pltpu.make_async_remote_copy(
                src_ref=s, dst_ref=dst.at[b, r], send_sem=sems[i],
                recv_sem=z_sem.at[b, ch * 2 + i], device_id=target, device_id_type=MESH))
        return out

    z_pending = []

    def z_send(b, ch, at, own):
        sems = [new_sem(), new_sem()]
        to = at + routes[b][0]

        @pl.when(z == at)
        def _():
            for c in z_copy(b, ch, dev(to, x, y, core), own, sems):
                c.start()
        z_pending.append((b, ch, at, own, sems))

    def z_arrive(b, ch, at):
        for c in z_copy(b, ch, (row, col), False, [send.at[0]] * 2):
            c.wait_recv()

    def z_round(hop, ch):
        for b in routes:
            if hop < routes[b][1]:
                at = b + routes[b][0] * hop

                @pl.when(z == at)
                def _():
                    z_arrive(b, ch, at)
                z_send(b, ch, at, False)

    def xm(d):
        return (x + d) % nx

    def ym(d):
        return (y + d) % ny

    other = (core + 1) % nk
    A, B = 0, 1
    for ch in range(CHUNKS):
        for b in routes:
            z_send(b, ch, b, True)
    for d in range(1, nx):
        lev_send(me, A, dev(z, xm(d), y, core), True)
    for d in range(1, ny):
        lev_send(me, B, dev(z, x, ym(d), core), True)
    for d in range(1, nx):
        lev_send(me, B, dev(z, xm(d), y, core), True)
    for d in range(1, ny):
        lev_send(me, A, dev(z, x, ym(d), core), True)
    if nk > 1:
        for part in (A, B):
            lev_send(me, part, dev(z, x, y, other), True)

    def prep(k, xv, lv):
        rows = pl.ds(pl.multiple_of(k * blk, blk), blk)
        hi, lo = split(xv)
        RHI[rows, :] = hi
        RLO[rows, :] = lo
        RLB[rows, :] = lv.astype(F32).astype(BF16)
        NR[:, rows] = to_row(jnp.sum(xv * xv, axis=1, keepdims=True))

    def prep_chunk(xx, skip):
        def step(i, _):
            k = xx * n_col + (col + i) % n_col
            prep(k, RX[k], RL[k])
            return 0

        lax.fori_loop(skip, n_col, step, 0)

    span = pn.group * blk
    scale = -1.0 / (2.0 * pn.width)

    def tile(slot, xx, xv, lv, own):
        chi, clo = split(xv)
        nc = jnp.sum(xv * xv, axis=1, keepdims=True)
        l0 = lv[:, 0:1].astype(F32)
        proj = PROJ[slot]
        tot = TOT[slot:slot + 1, :]
        for j in range(n_col // pn.group):
            base = pl.multiple_of(xx * n_col * blk + j * span, span)
            rows = pl.ds(base, span)
            hi, lo, lb = RHI[rows, :], RLO[rows, :], RLB[rows, :]
            dots = nt(chi, hi) + nt(chi, lo) + nt(clo, hi)
            dist = jnp.maximum(nc + NR[:, rows] - 2.0 * dots, 0.0)
            kern = jnp.exp(dist * scale)
            if own:
                ids = lax.broadcasted_iota(jnp.int32, (blk, span), 1) + base
                mine = lax.broadcasted_iota(jnp.int32, (blk, span), 0) + me * blk
                kern = jnp.where(ids == mine, 0.0, kern)
            kh, kl = split(kern)
            proj = proj + nn(kh, lb) + nn(kl, lb)
            t = jnp.sum(kern, axis=0, keepdims=True)
            for g in range(pn.group):
                tot = tot + t[:, g * blk:(g + 1) * blk]
            if not own:
                ROWP[:, rows] += jnp.sum(kern * l0, axis=0, keepdims=True)
        PROJ[slot] = proj
        TOT[slot:slot + 1, :] = tot

    def line_tiles(hop, chunks, arrive):
        for b in routes:
            if hop <= routes[b][1]:
                at = b + routes[b][0] * hop

                @pl.when(z == at)
                def _():
                    if arrive and hop == routes[b][1]:
                        for ch in range(CHUNKS):
                            z_arrive(b, ch, at)
                    for xx in chunks:
                        tile(b, xx, CX[b], CL[b], False)

    def own_tile(xx):
        tile(nz, xx, x_ref[...], l_ref[...], True)

    prep(me, x_ref[...], l_ref[...])
    ROWP[...] = jnp.zeros_like(ROWP)
    PROJ[...] = jnp.zeros_like(PROJ)
    TOT[...] = jnp.zeros_like(TOT)

    def partner(k, part):
        if nk > 1:
            lev_send(k, part, dev(z, x, y, other))

    z_round(1, 0)
    for d in range(1, nx):
        k = lev_of(xm(d), y, core)
        lev_wait(k, A)
        for e in range(1, ny):
            lev_send(k, A, dev(z, x, ym(e), core))
        partner(k, A)
    for d in range(1, ny):
        k = lev_of(x, ym(d), core)
        lev_wait(k, B)
        for e in range(1, nx):
            lev_send(k, B, dev(z, xm(e), y, core))
        partner(k, B)
    z_round(1, 1)
    z_round(2, 0)
    z_round(1, 2)
    z_round(2, 1)
    z_round(1, 3)
    for d in range(1, ny):
        k = lev_of(x, ym(d), core)
        lev_wait(k, A)
        partner(k, A)
    for d in range(1, nx):
        k = lev_of(xm(d), y, core)
        lev_wait(k, B)
        partner(k, B)
    z_round(2, 2)

    def other_core(xx, ys):
        if nk > 1:
            for e in ys:
                for part in (A, B):
                    lev_wait(lev_of(xx, ym(e), other), part)

    other_core(x, range(ny))
    prep_chunk(x, 1)
    own_tile(x)
    z_round(2, 3)
    line_tiles(1, [x], True)
    for d in range(1, nx):
        for e in range(1, ny):
            k = lev_of(xm(d), ym(e), core)
            for part in (A, B):
                lev_wait(k, part)
                partner(k, part)
    far = [xm(d) for d in range(1, nx)]
    for xx in far:
        other_core(xx, range(ny))
        prep_chunk(xx, 0)
        own_tile(xx)
    line_tiles(1, far, False)
    for hop in range(2, nz):
        line_tiles(hop, [x] + far, True)

    quad = jnp.zeros((1, pn.perms), F32)
    tot = jnp.zeros((1, blk), F32)
    for b in list(routes) + [nz]:
        w = 1.0 if b == nz else 2.0
        lv = l_ref[...] if b == nz else CL[b]
        QUAD[b:b + 1, :] = jnp.zeros((1, pn.perms), F32)
        COLP[b:b + 1, :] = jnp.zeros((1, blk), F32)
        reach = [nz - 1] if b == nz else [b + routes[b][0] * h for h in range(1, routes[b][1] + 1)]

        @pl.when((z >= (0 if b == nz else min(reach))) & (z <= max(reach)))
        def _():
            QUAD[b:b + 1, :] = w * jnp.sum(lv.astype(F32) * PROJ[b], axis=0, keepdims=True)
            COLP[b:b + 1, :] = to_row(PROJ[b][:, 0:1])
        quad = quad + QUAD[b:b + 1, :]
        tot = tot + w * TOT[b:b + 1, :]
    own_proof = COLP[nz:nz + 1, :]

    qr = pn.perms // 128
    for k in range(n_lev):
        for i in range(qr):
            S1[k, i:i + 1, :] = quad[:, i * 128:(i + 1) * 128]
        S1[k, qr:qr + 1, :] = tot
        S1[k, qr + 1:qr + 2, :] = ROWP[:, k * blk:(k + 1) * blk]
        S1[k, qr + 2:, :] = jnp.zeros((S1.shape[1] - qr - 2, 128), F32)

    def s1_copy(d):
        k = (me + d) % n_lev
        return pltpu.make_async_remote_copy(
            src_ref=S1.at[k], dst_ref=R1.at[me], send_sem=s1_send.at[k], recv_sem=s1_recv.at[me],
            device_id=lev_dev(k), device_id_type=MESH)

    def s1_in(d):
        k = (me + d) % n_lev
        return pltpu.make_async_remote_copy(
            src_ref=S1.at[k], dst_ref=R1.at[k], send_sem=s1_send.at[k], recv_sem=s1_recv.at[k],
            device_id=lev_dev(k), device_id_type=MESH)

    for d in range(1, n_lev):
        s1_copy(d).start()
    acc = S1[me]
    for d in range(1, n_lev):
        s1_in(d).wait_recv()
        acc = acc + R1[(me + d) % n_lev]
    for b in range(nz):
        S2[b, :, :] = acc
        S2[b, qr + 1:qr + 2, :] = COLP[b:b + 1, :] if b in routes else jnp.zeros((1, 128), F32)

    def s2_copy(d):
        b = (z + d) % nz
        return pltpu.make_async_remote_copy(
            src_ref=S2.at[b], dst_ref=R2.at[z], send_sem=s2_send.at[b], recv_sem=s2_recv.at[z],
            device_id=dev(b, x, y, core), device_id_type=MESH)

    def s2_in(d):
        b = (z + d) % nz
        return pltpu.make_async_remote_copy(
            src_ref=S2.at[b], dst_ref=R2.at[b], send_sem=s2_send.at[b], recv_sem=s2_recv.at[b],
            device_id=dev(b, x, y, core), device_id_type=MESH)

    for d in range(1, nz):
        s2_copy(d).start()
    for d in range(1, nz):
        s2_in(d).wait_recv()
    tops = []
    extra = jnp.zeros((1, 128), F32)
    for b in range(nz):
        mine = z == b
        tops.append(jnp.where(mine, acc, R2[b]))
        extra = extra + jnp.where(mine, 0.0, R2[b, qr + 1:qr + 2, :])
    done = functools.reduce(lambda u, v: u + v, tops)
    proof = acc[qr + 1:qr + 2, :] + own_proof + extra
    total = jnp.sum(done[qr:qr + 1, :], axis=1, keepdims=True)
    hf = pn.rows / 2.0
    den = 2.0 * hf * (hf - 1.0)
    stat = total / den + ((2.0 * hf - 1.0) / den) * done[0:qr, :]
    stat_ref[...] = stat
    proof_ref[...] = proof / math.sqrt(pn.rows)
    sg = 1.0 / (1.0 + jnp.exp(-4.0 * (stat - stat[0:1, 0:1])))
    first = (lax.broadcasted_iota(jnp.int32, stat.shape, 0) + lax.broadcasted_iota(jnp.int32, stat.shape, 1)) == 0
    sg = jnp.where(first, 0.0, sg)
    p = jnp.sum(jnp.sum(sg, axis=0, keepdims=True), axis=1, keepdims=True) / (pn.perms - 1)
    p_ref[...] = p

    for c in pending:
        c.wait_send()
    for b, ch, at, own, sems in z_pending:
        @pl.when(z == at)
        def _():
            for c in z_copy(b, ch, dev(at + routes[b][0], x, y, core), own, sems):
                c.wait_send()
    for d in range(1, n_lev):
        s1_copy(d).wait_send()
    for d in range(1, nz):
        s2_copy(d).wait_send()
    assert counter[0] == n_send


def send_count(pn):
    nx, ny, nk, nz = pn.nx, pn.ny, pn.nk, pn.nz
    own = 2 * (nx - 1) + 2 * (ny - 1) + (2 if nk > 1 else 0)
    fwd = 2 * (nx - 1) * (ny - 1)
    core = 2 * (nx * ny - 1) if nk > 1 else 0
    line = sum(h for _, h in ROUTES[nz].values()) * CHUNKS
    return 2 * (own + fwd + core + line)


def solution(mesh):
    n_row, n_col = mesh.shape["row"], mesh.shape["col"]

    def shards(samples, labels):
        blk, width = samples.shape
        perms = labels.shape[1]
        pn = Plan(n_row, n_col, blk, width, perms)
        n_send = send_count(pn)
        n_lev, nz = pn.n_lev, pn.nz
        vm = pl.BlockSpec(memory_space=pltpu.VMEM)
        dma = pltpu.SemaphoreType.DMA
        stat, proof, p = pl.pallas_call(
            functools.partial(kernel, pn, n_send),
            out_shape=(
                jax.ShapeDtypeStruct((perms // 128, 128), F32),
                jax.ShapeDtypeStruct((1, blk), F32),
                jax.ShapeDtypeStruct((1, 1), F32),
            ),
            in_specs=[vm, vm],
            out_specs=(vm, vm, vm),
            scratch_shapes=[
                pltpu.VMEM((n_lev, blk, width), F32),
                pltpu.VMEM((n_lev, blk, perms), jnp.int32),
                pltpu.VMEM((nz, blk, width), F32),
                pltpu.VMEM((nz, blk, perms), jnp.int32),
                pltpu.VMEM((n_lev * blk, width), BF16),
                pltpu.VMEM((n_lev * blk, width), BF16),
                pltpu.VMEM((n_lev * blk, perms), BF16),
                pltpu.VMEM((1, n_lev * blk), F32),
                pltpu.VMEM((1, n_lev * blk), F32),
                pltpu.VMEM((nz + 1, blk, perms), F32),
                pltpu.VMEM((nz + 1, perms), F32),
                pltpu.VMEM((nz + 1, blk), F32),
                pltpu.VMEM((nz + 1, blk), F32),
                pltpu.VMEM((n_lev, 8, 128), F32),
                pltpu.VMEM((n_lev, 8, 128), F32),
                pltpu.VMEM((nz, 8, 128), F32),
                pltpu.VMEM((nz, 8, 128), F32),
                dma((n_send,)),
                dma((n_lev, 2 * PARTS)),
                dma((nz, 2 * CHUNKS)),
                dma((n_lev,)),
                dma((n_lev,)),
                dma((nz,)),
                dma((nz,)),
            ],
            compiler_params=pltpu.CompilerParams(
                collective_id=0, has_side_effects=True, vmem_limit_bytes=60 * 1024 * 1024
            ),
        )(samples, labels)
        return stat.reshape(perms), proof.reshape(blk), p.reshape(())

    placed = (P(("row", "col"), None), P(("row", "col"), None))
    return jax.shard_map(
        shards, mesh=mesh, in_specs=placed, out_specs=(P(), P(("row", "col")), P()), check_vma=False
    )
```

```python
import functools
import math

import jax
import jax.numpy as jnp
from jax import lax
from jax.experimental import pallas as pl
from jax.experimental.pallas import tpu as pltpu
from jax.sharding import PartitionSpec as P

MESH = pl.DeviceIdType.MESH
F32 = jnp.float32
BF16 = jnp.bfloat16
CHUNKS = 4
PARTS = 2

ROUTES = {1: {}, 2: {0: (1, 1)}, 4: {0: (1, 3), 2: (-1, 1), 3: (-1, 2)}}


def nt(a, b):
    return lax.dot_general(a, b, (((1,), (1,)), ((), ())), preferred_element_type=F32)


def nn(a, b):
    return lax.dot_general(a, b, (((1,), (0,)), ((), ())), preferred_element_type=F32)


def split(v):
    hi = v.astype(BF16)
    return hi, (v - hi.astype(F32)).astype(BF16)


def to_row(column):
    n = column.shape[0]
    return jnp.transpose(jnp.broadcast_to(column, (n, n)))[0:1, :]


class Plan:
    def __init__(self, n_row, n_col, blk, width, perms):
        self.nz = math.gcd(n_row, 4)
        self.nx = n_row // self.nz
        self.nk = math.gcd(n_col, 2)
        self.ny = n_col // self.nk
        self.n_col = n_col
        self.n_lev = self.nx * n_col
        self.blk, self.width, self.perms = blk, width, perms
        self.direct = n_row * n_col <= 32
        self.group = math.gcd(n_col, 4)
        self.rows = blk * n_row * n_col


def kernel(pn, n_send, x_ref, l_ref, stat_ref, proof_ref, p_ref, RX, RL, CX, CL, RHI, RLO, RLB, NR,
           ROWP, PROJ, QUAD, TOT, COLP, S1, R1, S2, R2, send, lev_sem, z_sem, s1_send, s1_recv, s2_send, s2_recv, here):
    nx, ny, nz, nk, n_col, n_lev, blk = pn.nx, pn.ny, pn.nz, pn.nk, pn.n_col, pn.n_lev, pn.blk
    row, col = lax.axis_index("row"), lax.axis_index("col")
    z, x = row // nx, row % nx
    y, core = col // nk, col % nk
    me = x * n_col + col
    routes = ROUTES[nz]
    pending = []

    def lev_of(xx, yy, kk):
        return xx * n_col + yy * nk + kk

    def dev(zz, xx, yy, kk):
        return (zz * nx + xx, yy * nk + kk)

    def lev_dev(k):
        return (z * nx + k // n_col, k % n_col)

    barrier = pltpu.get_barrier_semaphore()
    for d in range(1, n_lev):
        pl.semaphore_signal(barrier, inc=1, device_id=lev_dev((me + d) % n_lev), device_id_type=MESH)
    for d in range(1, nz):
        pl.semaphore_signal(barrier, inc=1, device_id=dev((z + d) % nz, x, y, core), device_id_type=MESH)
    pl.semaphore_wait(barrier, n_lev - 1 + nz - 1)

    n_dev = nz * n_lev
    direct = pn.direct
    if direct:
        for d in range(1, nz):
            pl.semaphore_signal(here, inc=1, device_id=dev((z + d) % nz, x, y, core), device_id_type=MESH)

    counter = [0]

    def new_sem():
        counter[0] += 1
        return send.at[counter[0] - 1]

    half = blk // PARTS
    piece = blk // CHUNKS

    def lev_copy(k, part, target, own, sem):
        r = pl.ds(part * half, half)
        out = []
        for i, (src, dst) in enumerate(((x_ref, RX), (l_ref, RL))):
            s = src.at[r] if own else dst.at[k, r]
            out.append(pltpu.make_async_remote_copy(
                src_ref=s, dst_ref=dst.at[k, r], send_sem=new_sem() if sem else send.at[0],
                recv_sem=lev_sem.at[k, part * 2 + i], device_id=target, device_id_type=MESH))
        return out

    def lev_send(k, part, target, own=False):
        for c in lev_copy(k, part, target, own, True):
            c.start()
            pending.append(c)

    def lev_wait(k, part):
        for c in lev_copy(k, part, (row, col), False, False):
            c.wait_recv()

    def z_copy(b, ch, target, own, sems):
        r = pl.ds(ch * piece, piece)
        out = []
        for i, (src, dst) in enumerate(((x_ref, CX), (l_ref, CL))):
            s = src.at[r] if own else dst.at[b, r]
            out.append(pltpu.make_async_remote_copy(
                src_ref=s, dst_ref=dst.at[b, r], send_sem=sems[i],
                recv_sem=z_sem.at[b, ch * 2 + i], device_id=target, device_id_type=MESH))
        return out

    z_pending = []

    def z_send(b, ch, at, own):
        sems = [new_sem(), new_sem()]
        to = at + routes[b][0]

        @pl.when(z == at)
        def _():
            for c in z_copy(b, ch, dev(to, x, y, core), own, sems):
                c.start()
        z_pending.append((b, ch, at, own, sems))

    def z_arrive(b, ch, at):
        for c in z_copy(b, ch, (row, col), False, [send.at[0]] * 2):
            c.wait_recv()

    def z_round(hop, ch):
        for b in routes:
            if hop < routes[b][1]:
                at = b + routes[b][0] * hop

                @pl.when(z == at)
                def _():
                    z_arrive(b, ch, at)
                z_send(b, ch, at, False)

    def xm(d):
        return (x + d) % nx

    def ym(d):
        return (y + d) % ny

    other = (core + 1) % nk
    A, B = 0, 1
    for ch in range(CHUNKS):
        for b in routes:
            z_send(b, ch, b, True)
    for d in range(1, nx):
        lev_send(me, A, dev(z, xm(d), y, core), True)
    for d in range(1, ny):
        lev_send(me, B, dev(z, x, ym(d), core), True)
    for d in range(1, nx):
        lev_send(me, B, dev(z, xm(d), y, core), True)
    for d in range(1, ny):
        lev_send(me, A, dev(z, x, ym(d), core), True)
    if nk > 1:
        for part in (A, B):
            lev_send(me, part, dev(z, x, y, other), True)

    def prep(k, xv, lv):
        rows = pl.ds(pl.multiple_of(k * blk, blk), blk)
        hi, lo = split(xv)
        RHI[rows, :] = hi
        RLO[rows, :] = lo
        RLB[rows, :] = lv.astype(F32).astype(BF16)
        NR[:, rows] = to_row(jnp.sum(xv * xv, axis=1, keepdims=True))

    def prep_chunk(xx, skip):
        def step(i, _):
            k = xx * n_col + (col + i) % n_col
            prep(k, RX[k], RL[k])
            return 0

        lax.fori_loop(skip, n_col, step, 0)

    span = pn.group * blk
    scale = -1.0 / (2.0 * pn.width)

    def tile(slot, xx, xv, lv, own):
        chi, clo = split(xv)
        nc = jnp.sum(xv * xv, axis=1, keepdims=True)
        l0 = lv[:, 0:1].astype(F32)
        proj = PROJ[slot]
        tot = TOT[slot:slot + 1, :]
        for j in range(n_col // pn.group):
            base = pl.multiple_of(xx * n_col * blk + j * span, span)
            rows = pl.ds(base, span)
            hi, lo, lb = RHI[rows, :], RLO[rows, :], RLB[rows, :]
            dots = nt(chi, hi) + nt(chi, lo) + nt(clo, hi)
            dist = jnp.maximum(nc + NR[:, rows] - 2.0 * dots, 0.0)
            kern = jnp.exp(dist * scale)
            if own:
                ids = lax.broadcasted_iota(jnp.int32, (blk, span), 1) + base
                mine = lax.broadcasted_iota(jnp.int32, (blk, span), 0) + me * blk
                kern = jnp.where(ids == mine, 0.0, kern)
            kh, kl = split(kern)
            proj = proj + nn(kh, lb) + nn(kl, lb)
            t = jnp.sum(kern, axis=0, keepdims=True)
            for g in range(pn.group):
                tot = tot + t[:, g * blk:(g + 1) * blk]
            if not own:
                ROWP[:, rows] += jnp.sum(kern * l0, axis=0, keepdims=True)
        PROJ[slot] = proj
        TOT[slot:slot + 1, :] = tot

    def line_tiles(hop, chunks, arrive):
        for b in routes:
            if hop <= routes[b][1]:
                at = b + routes[b][0] * hop

                @pl.when(z == at)
                def _():
                    if arrive and hop == routes[b][1]:
                        for ch in range(CHUNKS):
                            z_arrive(b, ch, at)
                    for xx in chunks:
                        tile(b, xx, CX[b], CL[b], False)

    def own_tile(xx):
        tile(nz, xx, x_ref[...], l_ref[...], True)

    prep(me, x_ref[...], l_ref[...])
    ROWP[...] = jnp.zeros_like(ROWP)
    PROJ[...] = jnp.zeros_like(PROJ)
    TOT[...] = jnp.zeros_like(TOT)

    def partner(k, part):
        if nk > 1:
            lev_send(k, part, dev(z, x, y, other))

    z_round(1, 0)
    for d in range(1, nx):
        k = lev_of(xm(d), y, core)
        lev_wait(k, A)
        for e in range(1, ny):
            lev_send(k, A, dev(z, x, ym(e), core))
        partner(k, A)
    for d in range(1, ny):
        k = lev_of(x, ym(d), core)
        lev_wait(k, B)
        for e in range(1, nx):
            lev_send(k, B, dev(z, xm(e), y, core))
        partner(k, B)
    z_round(1, 1)
    z_round(2, 0)
    z_round(1, 2)
    z_round(2, 1)
    z_round(1, 3)
    for d in range(1, ny):
        k = lev_of(x, ym(d), core)
        lev_wait(k, A)
        partner(k, A)
    for d in range(1, nx):
        k = lev_of(xm(d), y, core)
        lev_wait(k, B)
        partner(k, B)
    z_round(2, 2)

    def other_core(xx, ys):
        if nk > 1:
            for e in ys:
                for part in (A, B):
                    lev_wait(lev_of(xx, ym(e), other), part)

    other_core(x, range(ny))
    prep_chunk(x, 1)
    own_tile(x)
    z_round(2, 3)
    line_tiles(1, [x], True)
    for d in range(1, nx):
        for e in range(1, ny):
            k = lev_of(xm(d), ym(e), core)
            for part in (A, B):
                lev_wait(k, part)
                partner(k, part)
    far = [xm(d) for d in range(1, nx)]
    for xx in far:
        other_core(xx, range(ny))
        prep_chunk(xx, 0)
        own_tile(xx)
    line_tiles(1, far, False)
    for hop in range(2, nz):
        line_tiles(hop, [x] + far, True)

    quad = jnp.zeros((1, pn.perms), F32)
    tot = jnp.zeros((1, blk), F32)
    for b in list(routes) + [nz]:
        w = 1.0 if b == nz else 2.0
        lv = l_ref[...] if b == nz else CL[b]
        QUAD[b:b + 1, :] = jnp.zeros((1, pn.perms), F32)
        COLP[b:b + 1, :] = jnp.zeros((1, blk), F32)
        reach = [nz - 1] if b == nz else [b + routes[b][0] * h for h in range(1, routes[b][1] + 1)]

        @pl.when((z >= (0 if b == nz else min(reach))) & (z <= max(reach)))
        def _():
            QUAD[b:b + 1, :] = w * jnp.sum(lv.astype(F32) * PROJ[b], axis=0, keepdims=True)
            COLP[b:b + 1, :] = to_row(PROJ[b][:, 0:1])
        quad = quad + QUAD[b:b + 1, :]
        tot = tot + w * TOT[b:b + 1, :]
    own_proof = COLP[nz:nz + 1, :]

    qr = pn.perms // 128
    if direct:
        def head(ref, i):
            for j in range(qr):
                ref[i, j:j + 1, :] = quad[:, j * 128:(j + 1) * 128]
            ref[i, qr:qr + 1, :] = tot

        index = z * n_lev + me
        none = jnp.zeros((1, 128), F32)
        for k in range(n_lev):
            head(S1, k)
            S1[k, qr + 1:qr + 2, :] = ROWP[:, k * blk:(k + 1) * blk]
        for b in range(nz):
            head(S2, b)
            S2[b, qr + 1:qr + 2, :] = COLP[b:b + 1, :] if b in routes else none
        head(S2, nz)
        S2[nz, qr + 1:qr + 2, :] = none
        if nz > 1:
            pl.semaphore_wait(here, nz - 1)

        def x_copy(dz, d, slot):
            b, k = (z + dz) % nz, (me + d) % n_lev
            src = S1.at[k] if dz == 0 else (S2.at[b] if d == 0 else S2.at[nz])
            return pltpu.make_async_remote_copy(
                src_ref=src, dst_ref=R1.at[slot], send_sem=s1_send.at[dz * n_lev + d], recv_sem=s1_recv.at[slot],
                device_id=(b * nx + k // n_col, k % n_col), device_id_type=MESH)

        pairs = [(dz, d) for dz in reversed(range(nz)) for d in range(n_lev) if dz + d > 0]
        for dz, d in pairs:
            x_copy(dz, d, index).start()
        R1[index] = S1[me]
        for dz, d in pairs:
            x_copy(dz, d, ((z + dz) % nz) * n_lev + (me + d) % n_lev).wait_recv()
        done = R1[0]
        for i in range(1, n_dev):
            done = done + R1[i]
        proof = done[qr + 1:qr + 2, :] + own_proof
    else:
        for k in range(n_lev):
            for i in range(qr):
                S1[k, i:i + 1, :] = quad[:, i * 128:(i + 1) * 128]
            S1[k, qr:qr + 1, :] = tot
            S1[k, qr + 1:qr + 2, :] = ROWP[:, k * blk:(k + 1) * blk]

        def s1_copy(d):
            k = (me + d) % n_lev
            return pltpu.make_async_remote_copy(
                src_ref=S1.at[k], dst_ref=R1.at[me], send_sem=s1_send.at[k], recv_sem=s1_recv.at[me],
                device_id=lev_dev(k), device_id_type=MESH)

        def s1_in(d):
            k = (me + d) % n_lev
            return pltpu.make_async_remote_copy(
                src_ref=S1.at[k], dst_ref=R1.at[k], send_sem=s1_send.at[k], recv_sem=s1_recv.at[k],
                device_id=lev_dev(k), device_id_type=MESH)

        for d in range(1, n_lev):
            s1_copy(d).start()
        acc = S1[me]
        for d in range(1, n_lev):
            s1_in(d).wait_recv()
            acc = acc + R1[(me + d) % n_lev]
        for b in range(nz):
            S2[b, :, :] = acc
            S2[b, qr + 1:qr + 2, :] = COLP[b:b + 1, :] if b in routes else jnp.zeros((1, 128), F32)

        def s2_copy(d):
            b = (z + d) % nz
            return pltpu.make_async_remote_copy(
                src_ref=S2.at[b], dst_ref=R2.at[z], send_sem=s2_send.at[b], recv_sem=s2_recv.at[z],
                device_id=dev(b, x, y, core), device_id_type=MESH)

        def s2_in(d):
            b = (z + d) % nz
            return pltpu.make_async_remote_copy(
                src_ref=S2.at[b], dst_ref=R2.at[b], send_sem=s2_send.at[b], recv_sem=s2_recv.at[b],
                device_id=dev(b, x, y, core), device_id_type=MESH)

        for d in range(1, nz):
            s2_copy(d).start()
        for d in range(1, nz):
            s2_in(d).wait_recv()
        tops = []
        extra = jnp.zeros((1, 128), F32)
        for b in range(nz):
            mine = z == b
            tops.append(jnp.where(mine, acc, R2[b]))
            extra = extra + jnp.where(mine, 0.0, R2[b, qr + 1:qr + 2, :])
        done = functools.reduce(lambda u, v: u + v, tops)
        proof = acc[qr + 1:qr + 2, :] + own_proof + extra
    total = jnp.sum(done[qr:qr + 1, :], axis=1, keepdims=True)
    hf = pn.rows / 2.0
    den = 2.0 * hf * (hf - 1.0)
    stat = total / den + ((2.0 * hf - 1.0) / den) * done[0:qr, :]
    stat_ref[...] = stat
    proof_ref[...] = proof / math.sqrt(pn.rows)
    sg = 1.0 / (1.0 + jnp.exp(-4.0 * (stat - stat[0:1, 0:1])))
    first = (lax.broadcasted_iota(jnp.int32, stat.shape, 0) + lax.broadcasted_iota(jnp.int32, stat.shape, 1)) == 0
    sg = jnp.where(first, 0.0, sg)
    p = jnp.sum(jnp.sum(sg, axis=0, keepdims=True), axis=1, keepdims=True) / (pn.perms - 1)
    p_ref[...] = p

    for c in pending:
        c.wait_send()
    for b, ch, at, own, sems in z_pending:
        @pl.when(z == at)
        def _():
            for c in z_copy(b, ch, dev(at + routes[b][0], x, y, core), own, sems):
                c.wait_send()
    if direct:
        for dz, d in pairs:
            x_copy(dz, d, index).wait_send()
    else:
        for d in range(1, n_lev):
            s1_copy(d).wait_send()
        for d in range(1, nz):
            s2_copy(d).wait_send()
    assert counter[0] == n_send


def send_count(pn):
    nx, ny, nk, nz = pn.nx, pn.ny, pn.nk, pn.nz
    own = 2 * (nx - 1) + 2 * (ny - 1) + (2 if nk > 1 else 0)
    fwd = 2 * (nx - 1) * (ny - 1)
    core = 2 * (nx * ny - 1) if nk > 1 else 0
    line = sum(h for _, h in ROUTES[nz].values()) * CHUNKS
    return 2 * (own + fwd + core + line)


def solution(mesh):
    n_row, n_col = mesh.shape["row"], mesh.shape["col"]

    def shards(samples, labels):
        blk, width = samples.shape
        perms = labels.shape[1]
        pn = Plan(n_row, n_col, blk, width, perms)
        n_send = send_count(pn)
        n_lev, nz = pn.n_lev, pn.nz
        msg = perms // 128 + 2
        slots = n_row * n_col if pn.direct else n_lev
        vm = pl.BlockSpec(memory_space=pltpu.VMEM)
        dma = pltpu.SemaphoreType.DMA
        stat, proof, p = pl.pallas_call(
            functools.partial(kernel, pn, n_send),
            out_shape=(
                jax.ShapeDtypeStruct((perms // 128, 128), F32),
                jax.ShapeDtypeStruct((1, blk), F32),
                jax.ShapeDtypeStruct((1, 1), F32),
            ),
            in_specs=[vm, vm],
            out_specs=(vm, vm, vm),
            scratch_shapes=[
                pltpu.VMEM((n_lev, blk, width), F32),
                pltpu.VMEM((n_lev, blk, perms), jnp.int32),
                pltpu.VMEM((nz, blk, width), F32),
                pltpu.VMEM((nz, blk, perms), jnp.int32),
                pltpu.VMEM((n_lev * blk, width), BF16),
                pltpu.VMEM((n_lev * blk, width), BF16),
                pltpu.VMEM((n_lev * blk, perms), BF16),
                pltpu.VMEM((1, n_lev * blk), F32),
                pltpu.VMEM((1, n_lev * blk), F32),
                pltpu.VMEM((nz + 1, blk, perms), F32),
                pltpu.VMEM((nz + 1, perms), F32),
                pltpu.VMEM((nz + 1, blk), F32),
                pltpu.VMEM((nz + 1, blk), F32),
                pltpu.VMEM((n_lev, msg, 128), F32),
                pltpu.VMEM((slots, msg, 128), F32),
                pltpu.VMEM((nz + 1, msg, 128), F32),
                pltpu.VMEM((nz, msg, 128), F32),
                dma((n_send,)),
                dma((n_lev, 2 * PARTS)),
                dma((nz, 2 * CHUNKS)),
                dma((slots,)),
                dma((slots,)),
                dma((nz,)),
                dma((nz,)),
                pltpu.SemaphoreType.REGULAR,
            ],
            compiler_params=pltpu.CompilerParams(
                collective_id=0, has_side_effects=True, vmem_limit_bytes=60 * 1024 * 1024
            ),
        )(samples, labels)
        return stat.reshape(perms), proof.reshape(blk), p.reshape(())

    placed = (P(("row", "col"), None), P(("row", "col"), None))
    return jax.shard_map(
        shards, mesh=mesh, in_specs=placed, out_specs=(P(), P(("row", "col")), P()), check_vma=False
    )
```

```python
import functools
import math

import jax
import jax.numpy as jnp
from jax import lax
from jax.experimental import pallas as pl
from jax.experimental.pallas import tpu as pltpu
from jax.sharding import PartitionSpec as P

MESH = pl.DeviceIdType.MESH
F32 = jnp.float32
BF16 = jnp.bfloat16
CHUNKS = 4
PARTS = 2

ROUTES = {1: {}, 2: {0: (1, 1)}, 4: {0: (1, 3), 2: (-1, 1), 3: (-1, 2)}}


def nt(a, b):
    return lax.dot_general(a, b, (((1,), (1,)), ((), ())), preferred_element_type=F32)


def nn(a, b):
    return lax.dot_general(a, b, (((1,), (0,)), ((), ())), preferred_element_type=F32)


def split(v):
    hi = v.astype(BF16)
    return hi, (v - hi.astype(F32)).astype(BF16)


def to_row(column):
    n = column.shape[0]
    return jnp.transpose(jnp.broadcast_to(column, (n, n)))[0:1, :]


class Plan:
    def __init__(self, n_row, n_col, blk, width, perms):
        self.nz = math.gcd(n_row, 4)
        self.nx = n_row // self.nz
        self.nk = math.gcd(n_col, 2)
        self.ny = n_col // self.nk
        self.n_col = n_col
        self.n_lev = self.nx * n_col
        self.blk, self.width, self.perms = blk, width, perms
        self.direct = n_row * n_col <= 32
        self.group = math.gcd(n_col, 4)
        self.rows = blk * n_row * n_col


def kernel(pn, n_send, x_hbm, l_hbm, stat_ref, proof_ref, p_ref, x_ref, l_ref, RX, RL, CX, CL, RHI, RLO, RLB, NR,
           ROWP, PROJ, QUAD, TOT, COLP, S1, R1, S2, R2, in_sem, send, lev_sem, z_sem, s1_send, s1_recv, s2_send, s2_recv, here):
    nx, ny, nz, nk, n_col, n_lev, blk = pn.nx, pn.ny, pn.nz, pn.nk, pn.n_col, pn.n_lev, pn.blk
    row, col = lax.axis_index("row"), lax.axis_index("col")
    z, x = row // nx, row % nx
    y, core = col // nk, col % nk
    me = x * n_col + col
    routes = ROUTES[nz]
    pending = []

    def lev_of(xx, yy, kk):
        return xx * n_col + yy * nk + kk

    def dev(zz, xx, yy, kk):
        return (zz * nx + xx, yy * nk + kk)

    def lev_dev(k):
        return (z * nx + k // n_col, k % n_col)

    loads = [pltpu.make_async_copy(x_hbm, x_ref, in_sem.at[0]), pltpu.make_async_copy(l_hbm, l_ref, in_sem.at[1])]
    for c in loads:
        c.start()
    barrier = pltpu.get_barrier_semaphore()
    for d in range(1, n_lev):
        pl.semaphore_signal(barrier, inc=1, device_id=lev_dev((me + d) % n_lev), device_id_type=MESH)
    for d in range(1, nz):
        pl.semaphore_signal(barrier, inc=1, device_id=dev((z + d) % nz, x, y, core), device_id_type=MESH)
    pl.semaphore_wait(barrier, n_lev - 1 + nz - 1)
    for c in loads:
        c.wait()

    n_dev = nz * n_lev
    direct = pn.direct
    if direct:
        for d in range(1, nz):
            pl.semaphore_signal(here, inc=1, device_id=dev((z + d) % nz, x, y, core), device_id_type=MESH)

    counter = [0]

    def new_sem():
        counter[0] += 1
        return send.at[counter[0] - 1]

    half = blk // PARTS
    piece = blk // CHUNKS

    def lev_copy(k, part, target, own, sem):
        r = pl.ds(part * half, half)
        out = []
        for i, (src, dst) in enumerate(((x_ref, RX), (l_ref, RL))):
            s = src.at[r] if own else dst.at[k, r]
            out.append(pltpu.make_async_remote_copy(
                src_ref=s, dst_ref=dst.at[k, r], send_sem=new_sem() if sem else send.at[0],
                recv_sem=lev_sem.at[k, part * 2 + i], device_id=target, device_id_type=MESH))
        return out

    def lev_send(k, part, target, own=False):
        for c in lev_copy(k, part, target, own, True):
            c.start()
            pending.append(c)

    def lev_wait(k, part):
        for c in lev_copy(k, part, (row, col), False, False):
            c.wait_recv()

    def z_copy(b, ch, target, own, sems):
        r = pl.ds(ch * piece, piece)
        out = []
        for i, (src, dst) in enumerate(((x_ref, CX), (l_ref, CL))):
            s = src.at[r] if own else dst.at[b, r]
            out.append(pltpu.make_async_remote_copy(
                src_ref=s, dst_ref=dst.at[b, r], send_sem=sems[i],
                recv_sem=z_sem.at[b, ch * 2 + i], device_id=target, device_id_type=MESH))
        return out

    z_pending = []

    def z_send(b, ch, at, own):
        sems = [new_sem(), new_sem()]
        to = at + routes[b][0]

        @pl.when(z == at)
        def _():
            for c in z_copy(b, ch, dev(to, x, y, core), own, sems):
                c.start()
        z_pending.append((b, ch, at, own, sems))

    def z_arrive(b, ch, at):
        for c in z_copy(b, ch, (row, col), False, [send.at[0]] * 2):
            c.wait_recv()

    def z_round(hop, ch):
        for b in routes:
            if hop < routes[b][1]:
                at = b + routes[b][0] * hop

                @pl.when(z == at)
                def _():
                    z_arrive(b, ch, at)
                z_send(b, ch, at, False)

    def xm(d):
        return (x + d) % nx

    def ym(d):
        return (y + d) % ny

    other = (core + 1) % nk
    A, B = 0, 1
    for ch in range(CHUNKS):
        for b in routes:
            z_send(b, ch, b, True)
    for d in range(1, nx):
        lev_send(me, A, dev(z, xm(d), y, core), True)
    for d in range(1, ny):
        lev_send(me, B, dev(z, x, ym(d), core), True)
    for d in range(1, nx):
        lev_send(me, B, dev(z, xm(d), y, core), True)
    for d in range(1, ny):
        lev_send(me, A, dev(z, x, ym(d), core), True)
    if nk > 1:
        for part in (A, B):
            lev_send(me, part, dev(z, x, y, other), True)

    def prep(k, xv, lv):
        rows = pl.ds(pl.multiple_of(k * blk, blk), blk)
        hi, lo = split(xv)
        RHI[rows, :] = hi
        RLO[rows, :] = lo
        RLB[rows, :] = lv.astype(F32).astype(BF16)
        NR[:, rows] = to_row(jnp.sum(xv * xv, axis=1, keepdims=True))

    def prep_chunk(xx, skip):
        def step(i, _):
            k = xx * n_col + (col + i) % n_col
            prep(k, RX[k], RL[k])
            return 0

        lax.fori_loop(skip, n_col, step, 0)

    span = pn.group * blk
    scale = -1.0 / (2.0 * pn.width)

    def tile(slot, xx, xv, lv, own):
        chi, clo = split(xv)
        nc = jnp.sum(xv * xv, axis=1, keepdims=True)
        l0 = lv[:, 0:1].astype(F32)
        proj = PROJ[slot]
        tot = TOT[slot:slot + 1, :]
        for j in range(n_col // pn.group):
            base = pl.multiple_of(xx * n_col * blk + j * span, span)
            rows = pl.ds(base, span)
            hi, lo, lb = RHI[rows, :], RLO[rows, :], RLB[rows, :]
            dots = nt(chi, hi) + nt(chi, lo) + nt(clo, hi)
            dist = jnp.maximum(nc + NR[:, rows] - 2.0 * dots, 0.0)
            kern = jnp.exp(dist * scale)
            if own:
                ids = lax.broadcasted_iota(jnp.int32, (blk, span), 1) + base
                mine = lax.broadcasted_iota(jnp.int32, (blk, span), 0) + me * blk
                kern = jnp.where(ids == mine, 0.0, kern)
            kh, kl = split(kern)
            proj = proj + nn(kh, lb) + nn(kl, lb)
            t = jnp.sum(kern, axis=0, keepdims=True)
            for g in range(pn.group):
                tot = tot + t[:, g * blk:(g + 1) * blk]
            if not own:
                ROWP[:, rows] += jnp.sum(kern * l0, axis=0, keepdims=True)
        PROJ[slot] = proj
        TOT[slot:slot + 1, :] = tot

    def line_tiles(hop, chunks, arrive):
        for b in routes:
            if hop <= routes[b][1]:
                at = b + routes[b][0] * hop

                @pl.when(z == at)
                def _():
                    if arrive and hop == routes[b][1]:
                        for ch in range(CHUNKS):
                            z_arrive(b, ch, at)
                    for xx in chunks:
                        tile(b, xx, CX[b], CL[b], False)

    def own_tile(xx):
        tile(nz, xx, x_ref[...], l_ref[...], True)

    prep(me, x_ref[...], l_ref[...])
    ROWP[...] = jnp.zeros_like(ROWP)
    PROJ[...] = jnp.zeros_like(PROJ)
    TOT[...] = jnp.zeros_like(TOT)

    def partner(k, part):
        if nk > 1:
            lev_send(k, part, dev(z, x, y, other))

    z_round(1, 0)
    for d in range(1, nx):
        k = lev_of(xm(d), y, core)
        lev_wait(k, A)
        for e in range(1, ny):
            lev_send(k, A, dev(z, x, ym(e), core))
        partner(k, A)
    for d in range(1, ny):
        k = lev_of(x, ym(d), core)
        lev_wait(k, B)
        for e in range(1, nx):
            lev_send(k, B, dev(z, xm(e), y, core))
        partner(k, B)
    z_round(1, 1)
    z_round(2, 0)
    z_round(1, 2)
    z_round(2, 1)
    z_round(1, 3)
    for d in range(1, ny):
        k = lev_of(x, ym(d), core)
        lev_wait(k, A)
        partner(k, A)
    for d in range(1, nx):
        k = lev_of(xm(d), y, core)
        lev_wait(k, B)
        partner(k, B)
    z_round(2, 2)

    def other_core(xx, ys):
        if nk > 1:
            for e in ys:
                for part in (A, B):
                    lev_wait(lev_of(xx, ym(e), other), part)

    other_core(x, range(ny))
    prep_chunk(x, 1)
    own_tile(x)
    z_round(2, 3)
    line_tiles(1, [x], True)
    for d in range(1, nx):
        for e in range(1, ny):
            k = lev_of(xm(d), ym(e), core)
            for part in (A, B):
                lev_wait(k, part)
                partner(k, part)
    far = [xm(d) for d in range(1, nx)]
    for xx in far:
        other_core(xx, range(ny))
        prep_chunk(xx, 0)
        own_tile(xx)
    line_tiles(1, far, False)
    for hop in range(2, nz):
        line_tiles(hop, [x] + far, True)

    quad = jnp.zeros((1, pn.perms), F32)
    tot = jnp.zeros((1, blk), F32)
    for b in list(routes) + [nz]:
        w = 1.0 if b == nz else 2.0
        lv = l_ref[...] if b == nz else CL[b]
        QUAD[b:b + 1, :] = jnp.zeros((1, pn.perms), F32)
        COLP[b:b + 1, :] = jnp.zeros((1, blk), F32)
        reach = [nz - 1] if b == nz else [b + routes[b][0] * h for h in range(1, routes[b][1] + 1)]

        @pl.when((z >= (0 if b == nz else min(reach))) & (z <= max(reach)))
        def _():
            QUAD[b:b + 1, :] = w * jnp.sum(lv.astype(F32) * PROJ[b], axis=0, keepdims=True)
            COLP[b:b + 1, :] = to_row(PROJ[b][:, 0:1])
        quad = quad + QUAD[b:b + 1, :]
        tot = tot + w * TOT[b:b + 1, :]
    own_proof = COLP[nz:nz + 1, :]

    qr = pn.perms // 128
    if direct:
        def head(ref, i):
            for j in range(qr):
                ref[i, j:j + 1, :] = quad[:, j * 128:(j + 1) * 128]
            ref[i, qr:qr + 1, :] = tot

        index = z * n_lev + me
        none = jnp.zeros((1, 128), F32)
        for k in range(n_lev):
            head(S1, k)
            S1[k, qr + 1:qr + 2, :] = ROWP[:, k * blk:(k + 1) * blk]
        for b in range(nz):
            head(S2, b)
            S2[b, qr + 1:qr + 2, :] = COLP[b:b + 1, :] if b in routes else none
        head(S2, nz)
        S2[nz, qr + 1:qr + 2, :] = none
        if nz > 1:
            pl.semaphore_wait(here, nz - 1)

        def x_copy(dz, d, slot):
            b, k = (z + dz) % nz, (me + d) % n_lev
            src = S1.at[k] if dz == 0 else (S2.at[b] if d == 0 else S2.at[nz])
            return pltpu.make_async_remote_copy(
                src_ref=src, dst_ref=R1.at[slot], send_sem=s1_send.at[dz * n_lev + d], recv_sem=s1_recv.at[slot],
                device_id=(b * nx + k // n_col, k % n_col), device_id_type=MESH)

        pairs = [(dz, d) for dz in reversed(range(nz)) for d in range(n_lev) if dz + d > 0]
        for dz, d in pairs:
            x_copy(dz, d, index).start()
        R1[index] = S1[me]
        for dz, d in pairs:
            x_copy(dz, d, ((z + dz) % nz) * n_lev + (me + d) % n_lev).wait_recv()
        done = R1[0]
        for i in range(1, n_dev):
            done = done + R1[i]
        proof = done[qr + 1:qr + 2, :] + own_proof
    else:
        for k in range(n_lev):
            for i in range(qr):
                S1[k, i:i + 1, :] = quad[:, i * 128:(i + 1) * 128]
            S1[k, qr:qr + 1, :] = tot
            S1[k, qr + 1:qr + 2, :] = ROWP[:, k * blk:(k + 1) * blk]

        def s1_copy(d):
            k = (me + d) % n_lev
            return pltpu.make_async_remote_copy(
                src_ref=S1.at[k], dst_ref=R1.at[me], send_sem=s1_send.at[k], recv_sem=s1_recv.at[me],
                device_id=lev_dev(k), device_id_type=MESH)

        def s1_in(d):
            k = (me + d) % n_lev
            return pltpu.make_async_remote_copy(
                src_ref=S1.at[k], dst_ref=R1.at[k], send_sem=s1_send.at[k], recv_sem=s1_recv.at[k],
                device_id=lev_dev(k), device_id_type=MESH)

        for d in range(1, n_lev):
            s1_copy(d).start()
        acc = S1[me]
        for d in range(1, n_lev):
            s1_in(d).wait_recv()
            acc = acc + R1[(me + d) % n_lev]
        for b in range(nz):
            S2[b, :, :] = acc
            S2[b, qr + 1:qr + 2, :] = COLP[b:b + 1, :] if b in routes else jnp.zeros((1, 128), F32)

        def s2_copy(d):
            b = (z + d) % nz
            return pltpu.make_async_remote_copy(
                src_ref=S2.at[b], dst_ref=R2.at[z], send_sem=s2_send.at[b], recv_sem=s2_recv.at[z],
                device_id=dev(b, x, y, core), device_id_type=MESH)

        def s2_in(d):
            b = (z + d) % nz
            return pltpu.make_async_remote_copy(
                src_ref=S2.at[b], dst_ref=R2.at[b], send_sem=s2_send.at[b], recv_sem=s2_recv.at[b],
                device_id=dev(b, x, y, core), device_id_type=MESH)

        for d in range(1, nz):
            s2_copy(d).start()
        for d in range(1, nz):
            s2_in(d).wait_recv()
        tops = []
        extra = jnp.zeros((1, 128), F32)
        for b in range(nz):
            mine = z == b
            tops.append(jnp.where(mine, acc, R2[b]))
            extra = extra + jnp.where(mine, 0.0, R2[b, qr + 1:qr + 2, :])
        done = functools.reduce(lambda u, v: u + v, tops)
        proof = acc[qr + 1:qr + 2, :] + own_proof + extra
    total = jnp.sum(done[qr:qr + 1, :], axis=1, keepdims=True)
    hf = pn.rows / 2.0
    den = 2.0 * hf * (hf - 1.0)
    stat = total / den + ((2.0 * hf - 1.0) / den) * done[0:qr, :]
    stat_ref[...] = stat
    proof_ref[...] = proof / math.sqrt(pn.rows)
    sg = 1.0 / (1.0 + jnp.exp(-4.0 * (stat - stat[0:1, 0:1])))
    first = (lax.broadcasted_iota(jnp.int32, stat.shape, 0) + lax.broadcasted_iota(jnp.int32, stat.shape, 1)) == 0
    sg = jnp.where(first, 0.0, sg)
    p = jnp.sum(jnp.sum(sg, axis=0, keepdims=True), axis=1, keepdims=True) / (pn.perms - 1)
    p_ref[...] = p

    for c in pending:
        c.wait_send()
    for b, ch, at, own, sems in z_pending:
        @pl.when(z == at)
        def _():
            for c in z_copy(b, ch, dev(at + routes[b][0], x, y, core), own, sems):
                c.wait_send()
    if direct:
        for dz, d in pairs:
            x_copy(dz, d, index).wait_send()
    else:
        for d in range(1, n_lev):
            s1_copy(d).wait_send()
        for d in range(1, nz):
            s2_copy(d).wait_send()
    assert counter[0] == n_send


def send_count(pn):
    nx, ny, nk, nz = pn.nx, pn.ny, pn.nk, pn.nz
    own = 2 * (nx - 1) + 2 * (ny - 1) + (2 if nk > 1 else 0)
    fwd = 2 * (nx - 1) * (ny - 1)
    core = 2 * (nx * ny - 1) if nk > 1 else 0
    line = sum(h for _, h in ROUTES[nz].values()) * CHUNKS
    return 2 * (own + fwd + core + line)


def solution(mesh):
    n_row, n_col = mesh.shape["row"], mesh.shape["col"]

    def shards(samples, labels):
        blk, width = samples.shape
        perms = labels.shape[1]
        pn = Plan(n_row, n_col, blk, width, perms)
        n_send = send_count(pn)
        n_lev, nz = pn.n_lev, pn.nz
        msg = perms // 128 + 2
        slots = n_row * n_col if pn.direct else n_lev
        vm = pl.BlockSpec(memory_space=pltpu.VMEM)
        hbm = pl.BlockSpec(memory_space=pl.ANY)
        dma = pltpu.SemaphoreType.DMA
        stat, proof, p = pl.pallas_call(
            functools.partial(kernel, pn, n_send),
            out_shape=(
                jax.ShapeDtypeStruct((perms // 128, 128), F32),
                jax.ShapeDtypeStruct((1, blk), F32),
                jax.ShapeDtypeStruct((1, 1), F32),
            ),
            in_specs=[hbm, hbm],
            out_specs=(vm, vm, vm),
            scratch_shapes=[
                pltpu.VMEM((blk, width), F32),
                pltpu.VMEM((blk, perms), jnp.int32),
                pltpu.VMEM((n_lev, blk, width), F32),
                pltpu.VMEM((n_lev, blk, perms), jnp.int32),
                pltpu.VMEM((nz, blk, width), F32),
                pltpu.VMEM((nz, blk, perms), jnp.int32),
                pltpu.VMEM((n_lev * blk, width), BF16),
                pltpu.VMEM((n_lev * blk, width), BF16),
                pltpu.VMEM((n_lev * blk, perms), BF16),
                pltpu.VMEM((1, n_lev * blk), F32),
                pltpu.VMEM((1, n_lev * blk), F32),
                pltpu.VMEM((nz + 1, blk, perms), F32),
                pltpu.VMEM((nz + 1, perms), F32),
                pltpu.VMEM((nz + 1, blk), F32),
                pltpu.VMEM((nz + 1, blk), F32),
                pltpu.VMEM((n_lev, msg, 128), F32),
                pltpu.VMEM((slots, msg, 128), F32),
                pltpu.VMEM((nz + 1, msg, 128), F32),
                pltpu.VMEM((nz, msg, 128), F32),
                dma((2,)),
                dma((n_send,)),
                dma((n_lev, 2 * PARTS)),
                dma((nz, 2 * CHUNKS)),
                dma((slots,)),
                dma((slots,)),
                dma((nz,)),
                dma((nz,)),
                pltpu.SemaphoreType.REGULAR,
            ],
            compiler_params=pltpu.CompilerParams(
                collective_id=0, has_side_effects=True, vmem_limit_bytes=60 * 1024 * 1024
            ),
        )(samples, labels)
        return stat.reshape(perms), proof.reshape(blk), p.reshape(())

    placed = (P(("row", "col"), None), P(("row", "col"), None))
    return jax.shard_map(
        shards, mesh=mesh, in_specs=placed, out_specs=(P(), P(("row", "col")), P()), check_vma=False
    )
```
